32 devices in a mesh: section: 4 (over y, core), expert: 8 (over z, x).
Axes of the slice: x: 2, y: 2, z: 4, core: 2. Of those that a mesh axis runs over, the one named last changes fastest.
Arguments:
- inputs: bfloat16 [4, 1024, 1024], P('section', 'expert'), may hold values from -6 to 6
- out_grads: bfloat16 [4, 1024, 1024], P('section', 'expert'), may hold values from -6 to 6
- expert_ids: int32 [4, 1024, 8], P('section', 'expert'), may hold values from 0 to 15, all different within a row; in each aligned block of 128 rows (0 to 127, 128 to 255, ..., all dimensions but the last counted through in order) at most 96 rows name the same one
- route_levels: int32 [4, 1024, 8], P('section', 'expert'), may hold values from 8 to 256
- w_gate: bfloat16 [4, 16, 1024, 384], P('section', 'expert'), may hold values from -0.1875 to 0.1875
- w_up: bfloat16 [4, 16, 1024, 384], P('section', 'expert'), may hold values from -0.1875 to 0.1875
- w_down: bfloat16 [4, 16, 384, 1024], P('section', 'expert'), may hold values from -0.3125 to 0.3125
Outputs:
- upstream: bfloat16 [4, 1024, 1024], P('section', 'expert')
- route_grad: bfloat16 [4, 1024, 8], P('section', 'expert')
- gate_update: bfloat16 [4, 16, 1024, 384], P('section', 'expert')
- up_update: bfloat16 [4, 16, 1024, 384], P('section', 'expert')
- down_update: bfloat16 [4, 16, 384, 1024], P('section', 'expert')
The draws below stay inside these ranges and needn't reach their ends.
Inputs may be any that keep to these rules, and one draw needn't show every extreme that they name: `expert_ids`: each token names 8 different experts; among the 128 tokens of one aligned block no expert is named more than 96 times.
All inputs are finite; a program needn't handle non-finite values.
Results may differ from the reference program's by a relative error of at most 0.0064.
Values may be sent and summed in bfloat16 or wider, within the bound.
No kernel may reach another device: no remote copies, remote signals or barrier semaphores. Data moves between devices by JAX's collectives and lax.ppermute only.
A program may use at most 128 MiB of HBM per device.

```python
import math
import jax
import jax.numpy as jnp
import numpy as np
from jax import lax

D = 1024
H = 384
TOPK = 8
TOK_DEV = 128
EXPERTS = 16
CAP = 96
SECTIONS = 4
TOKENS = 1024
N_EXPERT = 8


def set_ends(entries, own_key, least, high):
    shape = entries.shape
    index_at = [jax.random.randint(jax.random.fold_in(own_key, axis), (), 0, shape[axis]) for axis in range(len(shape))]
    entries = entries.at[tuple(index_at)].set(least)
    longest = shape.index(max(shape))
    index_at[longest] = (index_at[longest] + 1) % shape[longest]
    return entries.at[tuple(index_at)].set(high)


def block_scale(key, extent, split, least, high):
    factor_of = 1.0
    for position, blocks in split:
        heights = jax.random.uniform(jax.random.fold_in(jax.random.fold_in(key, 6), position), (blocks,), jnp.float32, least / len(split), high / len(split))
        factor_of = factor_of * jnp.repeat(jnp.exp(heights), extent[position] // blocks).reshape((-1,) + (1,) * (len(extent) - 1 - position))
    return factor_of


def routed_block(key, own, number, rows, number_of, top, reach, skew):
    ranking = jax.random.permutation(key, number_of)
    crowded, ordinary = shares(number_of, rows * top, reach, skew, True), shares(number_of, rows * top, reach, skew, False)
    places = jnp.arange(number_of)

    def named(sizes, rotation):
        used = int((sizes > 0).sum())
        fixed = max(1, used // 4)
        moved = fixed + (places - fixed + rotation * (used - fixed)) % max(1, number_of - fixed)
        return jnp.zeros((number_of,), jnp.int32).at[ranking[jnp.where(places < fixed, places, moved)]].set(jnp.asarray(sizes, jnp.int32))

    sizes = jnp.where(number % 4 == 0, named(crowded, number // 4), named(ordinary, number - number // 4 - 1))
    mixed = jax.random.permutation(jax.random.fold_in(own, 3), number_of)
    giver, receiver = mixed[0:number_of // 2 * 2:2], mixed[1:number_of // 2 * 2:2]
    room = jnp.minimum(sizes[giver] - 1, reach - sizes[receiver]) // 2
    room = jnp.where((giver == ranking[0]) | (receiver == ranking[0]) | (sizes[receiver] == 0), 0, jnp.maximum(room, 0))
    moved = jax.random.randint(jax.random.fold_in(own, 4), (number_of // 2,), 0, 1 << 20) % (room + 1)
    sizes = sizes.at[giver].add(-moved).at[receiver].add(moved)
    labels = jnp.searchsorted(jnp.cumsum(sizes), jnp.arange(rows * top), side="right").astype(jnp.int32)
    grid = labels.reshape(top, rows).T
    grid = grid[jax.random.permutation(jax.random.fold_in(own, 1), rows)]
    rotation = jax.random.randint(jax.random.fold_in(own, 2), (rows, 1), 0, top)
    return jnp.take_along_axis(grid, (jnp.arange(top)[None, :] + rotation) % top, axis=1)


def shares(number_of, total, reach, skew, full):
    portions = [(1 << 20) // math.isqrt(rank ** skew) + 1 for rank in range(1, number_of + 1)]
    largest = reach if full else min(reach, max(-(-total // number_of), total * portions[0] // sum(portions)))
    least = 1 if total - largest >= number_of - 1 else 0
    counts, spare = [largest] + [least] * (number_of - 1), total - largest - least * (number_of - 1)
    while spare > 0:
        candidates = [i for i in range(1, number_of) if counts[i] < largest] or [i for i in range(1, number_of) if counts[i] < reach]
        pool, budget = sum([portions[i] for i in candidates]), spare
        for i in candidates:
            extra = min(reach - counts[i], max(1, budget * portions[i] // pool), spare)
            counts[i] = counts[i] + extra
            spare = spare - extra
    return np.array(counts)


def gaussian(own_key, extent, deviation, most, cuts=(), kind=jnp.bfloat16):
    factor_of = block_scale(own_key, extent, cuts, -0.22, 0.18) if cuts else 1.0
    array = jax.random.normal(own_key, extent, jnp.float32) * deviation * factor_of
    return jnp.minimum(jnp.maximum(array, -most), most).astype(kind)


def setup_inputs(seed: int = 0) -> dict:
    keys = jax.random.split(jax.random.key(seed), 8)
    inputs = gaussian(keys[0], (SECTIONS, TOKENS, D), 1.0, 6.0, ((0, 4), (1, 8)))
    out_grads = gaussian(keys[1], (SECTIONS, TOKENS, D), 1.0, 6.0, ((0, 4), (1, 8)))
    expert_ids_keys = jax.random.split(jax.random.fold_in(keys[2], 1), SECTIONS * TOKENS // TOK_DEV)
    expert_ids_turns = jax.random.permutation(jax.random.fold_in(keys[2], 3), SECTIONS * TOKENS // TOK_DEV)
    expert_ids = jax.vmap(lambda own, number: routed_block(jax.random.fold_in(keys[2], 2), own, number, TOK_DEV, EXPERTS, TOPK, CAP, 2))(expert_ids_keys, expert_ids_turns).reshape((SECTIONS, TOKENS, TOPK))
    route_levels = set_ends(jax.random.randint(keys[3], (SECTIONS, TOKENS, TOPK), 8, 257), jax.random.fold_in(keys[3], 1), 8, 256).astype(jnp.int32)
    w_gate = gaussian(keys[4], (SECTIONS, EXPERTS, D, H), D ** -0.5, 0.1875, ((0, 4), (1, 8)))
    w_up = gaussian(keys[5], (SECTIONS, EXPERTS, D, H), D ** -0.5, 0.1875, ((0, 4), (1, 8)))
    w_down = gaussian(keys[6], (SECTIONS, EXPERTS, H, D), H ** -0.5, 0.3125, ((0, 4), (1, 8)))
    return {"inputs": inputs, "out_grads": out_grads, "expert_ids": expert_ids, "route_levels": route_levels, "w_gate": w_gate, "w_up": w_up, "w_down": w_down}


def flat_slots(expert_ids, experts_all, capacity):
    blocks = expert_ids.shape[0]
    flat_ids = expert_ids.reshape(blocks, -1).astype(jnp.int32)
    catalog = jnp.arange(experts_all, dtype=jnp.int32)
    onehot = (flat_ids[:, :, None] == catalog[None, None, :]).astype(jnp.int32)
    rank_table = (jnp.cumsum(onehot, axis=1) - 1).astype(jnp.int32)
    slot_of = jnp.sum(onehot * rank_table, axis=2).astype(jnp.int32)
    return (flat_ids * capacity + slot_of).astype(jnp.int32).reshape(expert_ids.shape)


def expert_backward(slot_inputs, slot_grads, slot_routes, w_gate, w_up, w_down):
    inputs_wide = slot_inputs.astype(jnp.float32)
    grads_wide = slot_grads.astype(jnp.float32)
    gate_wide = w_gate.astype(jnp.float32)
    up_wide = w_up.astype(jnp.float32)
    down_wide = w_down.astype(jnp.float32)
    gate_pre = jnp.einsum('esd,edh->esh', inputs_wide, gate_wide)
    up_pre = jnp.einsum('esd,edh->esh', inputs_wide, up_wide)
    sigmoid_gate = jax.nn.sigmoid(gate_pre)
    silu_gate = gate_pre * sigmoid_gate
    active = (silu_gate * up_pre).astype(jnp.bfloat16)
    active_wide = active.astype(jnp.float32)
    expert_out = jnp.einsum('esh,ehd->esd', active_wide, down_wide)
    route_part = jnp.sum(grads_wide * expert_out, axis=2).astype(jnp.bfloat16)
    weighted = (slot_routes.astype(jnp.float32)[:, :, None] * grads_wide).astype(jnp.bfloat16)
    weighted_wide = weighted.astype(jnp.float32)
    active_grad = jnp.einsum('esd,ehd->esh', weighted_wide, down_wide)
    gate_pre_grad = (active_grad * up_pre * sigmoid_gate * (1.0 + gate_pre * (1.0 - sigmoid_gate))).astype(jnp.bfloat16)
    up_pre_grad = (active_grad * silu_gate).astype(jnp.bfloat16)
    gate_grad_wide = gate_pre_grad.astype(jnp.float32)
    up_grad_wide = up_pre_grad.astype(jnp.float32)
    input_grad = (jnp.einsum('esh,edh->esd', gate_grad_wide, gate_wide)
                  + jnp.einsum('esh,edh->esd', up_grad_wide, up_wide)).astype(jnp.bfloat16)
    down_part = jnp.einsum('esh,esd->ehd', active_wide, weighted_wide).astype(jnp.bfloat16)
    gate_part = jnp.einsum('esd,esh->edh', inputs_wide, gate_grad_wide).astype(jnp.bfloat16)
    up_part = jnp.einsum('esd,esh->edh', inputs_wide, up_grad_wide).astype(jnp.bfloat16)
    return input_grad, route_part, gate_part, up_part, down_part


def section_backward(operands):
    inputs, out_grads, expert_ids, route_levels, w_gate, w_up, w_down = operands
    blocks = N_EXPERT
    flat_index = flat_slots(expert_ids.reshape(blocks, TOK_DEV, TOPK), EXPERTS, CAP)
    catalog = jnp.arange(EXPERTS * CAP, dtype=jnp.int32)
    select = (flat_index[..., None] == catalog).astype(jnp.float32).reshape(blocks, TOK_DEV, TOPK, EXPERTS, CAP)
    placing = jnp.sum(select, axis=2)
    route_values = (route_levels.astype(jnp.float32) / 256.0).reshape(blocks, TOK_DEV, TOPK)
    inputs_wide = inputs.astype(jnp.float32).reshape(blocks, TOK_DEV, D)
    grads_wide = out_grads.astype(jnp.float32).reshape(blocks, TOK_DEV, D)
    slot_inputs = jnp.einsum('btec,btd->ebcd', placing, inputs_wide).reshape(EXPERTS, blocks * CAP, D).astype(jnp.bfloat16)
    slot_grads = jnp.einsum('btec,btd->ebcd', placing, grads_wide).reshape(EXPERTS, blocks * CAP, D).astype(jnp.bfloat16)
    slot_routes = jnp.einsum('btkec,btk->ebc', select, route_values).reshape(EXPERTS, blocks * CAP).astype(jnp.bfloat16)
    input_grad, route_part, gate_part, up_part, down_part = expert_backward(slot_inputs, slot_grads, slot_routes, w_gate, w_up, w_down)
    back_inputs = input_grad.astype(jnp.float32).reshape(EXPERTS, blocks, CAP, D)
    token_grad = jnp.einsum('btec,ebcd->btd', placing, back_inputs).reshape(TOKENS, D).astype(jnp.bfloat16)
    back_routes = route_part.astype(jnp.float32).reshape(EXPERTS, blocks, CAP)
    token_route = jnp.einsum('btkec,ebc->btk', select, back_routes).reshape(TOKENS, TOPK).astype(jnp.bfloat16)
    return token_grad, token_route, gate_part, up_part, down_part


def reference(inputs, out_grads, expert_ids, route_levels, w_gate, w_up, w_down):
    token_grad, token_route, gate_part, up_part, down_part = lax.map(
        section_backward, (inputs, out_grads, expert_ids, route_levels, w_gate, w_up, w_down))
    upstream = jnp.concatenate([token_grad[1:], jnp.zeros_like(token_grad[:1])], axis=0)
    return upstream, token_route, gate_part, up_part, down_part
```

```python
import jax
import jax.numpy as jnp
from jax import lax
from jax.sharding import PartitionSpec as P

F32 = jnp.float32
BF16 = jnp.bfloat16


def ring_order(size):
    columns = 1
    while (2 * columns) ** 2 <= size and size % (2 * columns) == 0:
        columns *= 2
    rows = size // columns
    if columns == 1:
        return list(range(size))
    cells = [(0, 0)]
    for column in range(columns):
        span = range(1, rows) if column % 2 == 0 else range(rows - 1, 0, -1)
        cells += [(row, column) for row in span]
    cells += [(0, column) for column in range(columns - 1, 0, -1)]
    return [row * columns + column for row, column in cells]


def shifted(value, axis, by):
    size = lax.axis_size(axis)
    pairs = [(i, i + by) for i in range(size) if 0 <= i + by < size]
    return lax.ppermute(value, axis, pairs)


def block_backward(x, g, routes, w_in, w_down, experts_local):
    hidden = w_down.shape[0]
    each = hidden // experts_local
    pre = jnp.dot(x, w_in, preferred_element_type=F32)
    gate, up = pre[:, :hidden], pre[:, hidden:]
    back = lax.dot_general(g, w_down, (((1,), (1,)), ((), ())), preferred_element_type=F32)
    lane = lax.broadcasted_iota(jnp.int32, back.shape, 1) // each
    route = jnp.zeros(back.shape, F32)
    for e in range(experts_local):
        route = jnp.where(lane == e, routes[:, e][:, None], route)
    sig = jax.nn.sigmoid(gate)
    silu = gate * sig
    active = (silu * up).astype(BF16).astype(F32)
    scaled = (route * active).astype(BF16)
    grad = route * back
    gate_grad = (grad * up * sig * (1.0 + gate * (1.0 - sig))).astype(BF16)
    up_grad = (grad * silu).astype(BF16)
    product = active * back
    route_grad = jnp.stack(
        [jnp.sum(product[:, e * each:(e + 1) * each], axis=1) for e in range(experts_local)], axis=1
    )
    pre_grad = jnp.concatenate([gate_grad, up_grad], axis=1)
    part = lax.dot_general(pre_grad, w_in, (((1,), (1,)), ((), ())), preferred_element_type=F32)
    return part.astype(BF16), route_grad, pre_grad, scaled


def body(inputs, out_grads, expert_ids, route_levels, w_gate, w_up, w_down):
    x0, g0 = inputs[0], out_grads[0]
    ids = expert_ids[0]
    tokens, width = x0.shape
    experts_local, _, each = w_gate.shape[1:]
    groups = lax.axis_size("expert")
    experts_all = experts_local * groups
    half = groups // 2
    ring = ring_order(groups)
    fwd = [(ring[p], ring[(p + 1) % groups]) for p in range(groups)]
    bwd = [(b, a) for a, b in fwd]

    def go(value, pairs):
        return lax.ppermute(value, "expert", pairs)

    levels = route_levels[0].astype(F32) / 256.0
    catalog = jnp.arange(experts_all, dtype=jnp.int32)
    chosen = ids.T[None, :, :] == catalog[:, None, None]
    table = jnp.sum(jnp.where(chosen, levels.T[None], 0.0), axis=1).astype(BF16)
    received = lax.all_to_all(
        table.reshape(groups, experts_local, tokens), "expert", split_axis=0, concat_axis=0, tiled=True
    )
    ring_arr = jnp.array(ring, jnp.int32)
    me = lax.axis_index("expert")
    place = jnp.sum(jnp.where(ring_arr == me, jnp.arange(groups), 0))
    seat = jnp.sum(
        jnp.where(ring_arr[None, :] == jnp.arange(groups)[:, None], jnp.arange(groups)[None, :], 0), axis=1
    )
    turn = (
        jnp.mod(seat[None, :] - place, groups) == jnp.arange(groups)[:, None]
    ).astype(BF16)
    routes = jnp.dot(turn, received.reshape(groups, -1), preferred_element_type=F32)
    routes = routes.reshape(groups * experts_local, tokens).T

    w_in = jnp.concatenate(
        [w_gate[0, e] for e in range(experts_local)] + [w_up[0, e] for e in range(experts_local)], axis=1
    )
    w_out = w_down[0].reshape(experts_local * each, width)

    xs, gs = {0: x0}, {0: g0}
    xf = xb = x0
    gf = gb = g0
    for hop in range(1, half + 1):
        xf = go(xf, fwd)
        gb = go(gb, bwd)
        xs[groups - hop], gs[hop] = xf, gb
        if hop < half:
            gf = go(gf, fwd)
            xb = go(xb, bwd)
            gs[groups - hop], xs[hop] = gf, xb

    parts, route_grads, pre_grads, scaleds = {}, {}, {}, {}
    order = [0]
    for hop in range(1, half + 1):
        order += [hop] if hop == groups - hop else [hop, groups - hop]
    for o in order:
        mine = routes[:, o * experts_local:(o + 1) * experts_local]
        parts[o], route_grads[o], pre_grads[o], scaleds[o] = lax.optimization_barrier(
            block_backward(xs[o], gs[o], mine, w_in, w_out, experts_local)
        )

    cut = tokens // 2
    low = {o: parts[o][:cut] for o in parts}
    high = {o: parts[o][cut:] for o in parts}

    def chain(pieces, pairs, offsets):
        carried = None
        for o in offsets:
            piece = pieces[o]
            if carried is not None:
                piece = (carried.astype(F32) + piece.astype(F32)).astype(BF16)
            carried = go(piece, pairs)
        return carried

    longer = list(range(half, 0, -1))
    forward_low = chain(low, fwd, longer)
    backward_high = chain(high, bwd, [groups - o for o in longer])
    forward_high = chain(high, fwd, longer[1:])
    backward_low = chain(low, bwd, [groups - o for o in longer[1:]])

    def total(own, one, two):
        return (own.astype(F32) + one.astype(F32) + two.astype(F32)).astype(BF16)

    upstream = jnp.concatenate(
        [
            shifted(total(low[0], forward_low, backward_low), "section", -1),
            shifted(total(high[0], forward_high, backward_high), "section", -1),
        ],
        axis=0,
    )

    back_table = jnp.concatenate([route_grads[o] for o in range(groups)], axis=1).T.astype(BF16)
    back_table = lax.dot_general(
        turn, back_table.reshape(groups, -1), (((0,), (0,)), ((), ())), preferred_element_type=F32
    ).astype(BF16)
    returned = lax.all_to_all(
        back_table.reshape(groups, experts_local, tokens), "expert", split_axis=0, concat_axis=0, tiled=True
    ).reshape(experts_all, tokens)
    token_route = jnp.sum(jnp.where(chosen, returned.astype(F32)[:, None, :], 0.0), axis=0).T.astype(BF16)

    every = list(range(groups))
    all_x = jnp.concatenate([xs[o] for o in every], axis=0)
    all_g = jnp.concatenate([gs[o] for o in every], axis=0)
    all_pre = jnp.concatenate([pre_grads[o] for o in every], axis=0)
    all_scaled = jnp.concatenate([scaleds[o] for o in every], axis=0)
    rows = (((0,), (0,)), ((), ()))
    gate_part, up_part = [
        jnp.stack(
            [
                lax.dot_general(
                    all_x, all_pre[:, (s + e) * each:(s + e + 1) * each], rows, preferred_element_type=F32
                ).astype(BF16)
                for e in range(experts_local)
            ]
        )
        for s in (0, experts_local)
    ]
    down_part = (
        lax.dot_general(all_scaled, all_g, rows, preferred_element_type=F32)
        .astype(BF16)
        .reshape(experts_local, each, width)
    )
    return (upstream[None], token_route[None], gate_part[None], up_part[None], down_part[None])


def solution(mesh):
    in_specs = (
        P("section", "expert", None),
        P("section", "expert", None),
        P("section", "expert", None),
        P("section", "expert", None),
        P("section", "expert", None, None),
        P("section", "expert", None, None),
        P("section", "expert", None, None),
    )
    out_specs = (
        P("section", "expert", None),
        P("section", "expert", None),
        P("section", "expert", None, None),
        P("section", "expert", None, None),
        P("section", "expert", None, None),
    )
    return jax.shard_map(body, mesh=mesh, in_specs=in_specs, out_specs=out_specs, check_vma=False)
```

```python
import functools

import jax
import jax.numpy as jnp
from jax import lax
from jax.experimental import pallas as pl
from jax.experimental.pallas import tpu as pltpu
from jax.sharding import PartitionSpec as P

F32 = jnp.float32
BF16 = jnp.bfloat16
LAST = (((1,), (1,)), ((), ()))
ROWS = (((0,), (0,)), ((), ()))


def ring_order(size):
    columns = 1
    while (2 * columns) ** 2 <= size and size % (2 * columns) == 0:
        columns *= 2
    rows = size // columns
    if columns == 1:
        return list(range(size))
    cells = [(0, 0)]
    for column in range(columns):
        span = range(1, rows) if column % 2 == 0 else range(rows - 1, 0, -1)
        cells += [(row, column) for row in span]
    cells += [(0, column) for column in range(columns - 1, 0, -1)]
    return [row * columns + column for row, column in cells]


def shifted(value, axis, by):
    size = lax.axis_size(axis)
    pairs = [(i, i + by) for i in range(size) if 0 <= i + by < size]
    return lax.ppermute(value, axis, pairs)


def block_kernel(count, tokens, cut, *refs):
    first_ref, refs = refs[0], refs[1:]
    xs, gs, routes = refs[:count], refs[count:2 * count], refs[2 * count:3 * count]
    w_gate, w_up, w_down = refs[3 * count:3 * count + 3]
    outs = refs[3 * count + 3:]
    parts, (gate_out, up_out, scaled), (acc, table) = outs[:2 * count], outs[2 * count:-2], outs[-2:]
    experts_all = table.shape[1]
    e = pl.program_id(0)
    x = jnp.concatenate([ref[...] for ref in xs], axis=0)
    g = jnp.concatenate([ref[...] for ref in gs], axis=0)
    route = jnp.concatenate(
        [jnp.broadcast_to(ref[0], (tokens, tokens)).T[:, :1] for ref in routes], axis=0
    )
    gate = jnp.dot(x, w_gate[0], preferred_element_type=F32)
    up = jnp.dot(x, w_up[0], preferred_element_type=F32)
    back = lax.dot_general(g, w_down[0], LAST, preferred_element_type=F32)
    sig = jax.nn.sigmoid(gate)
    silu = gate * sig
    active = (silu * up).astype(BF16).astype(F32)
    scaled[0] = (route * active).astype(BF16)
    product = active * back
    coarse = product.astype(BF16)
    fine = (product - coarse.astype(F32)).astype(BF16)
    ones = jnp.ones((experts_all, product.shape[1]), BF16)
    row_grad = lax.dot_general(ones, coarse, LAST, preferred_element_type=F32) + lax.dot_general(
        ones, fine, LAST, preferred_element_type=F32
    )
    own_row = lax.broadcasted_iota(jnp.int32, (experts_all, tokens), 0) == first_ref[0] + e
    grad = route * back
    gate_grad = (grad * up * sig * (1.0 + gate * (1.0 - sig))).astype(BF16)
    up_grad = (grad * silu).astype(BF16)
    gate_out[0] = gate_grad
    up_out[0] = up_grad
    part = lax.dot_general(gate_grad, w_gate[0], LAST, preferred_element_type=F32) + lax.dot_general(
        up_grad, w_up[0], LAST, preferred_element_type=F32
    )

    @pl.when(e == 0)
    def _():
        acc[...] = part
        table[...] = jnp.zeros(table.shape, F32)

    @pl.when(e > 0)
    def _():
        acc[...] += part

    for i in range(count):
        table[i] = jnp.where(own_row, row_grad[:, i * tokens:(i + 1) * tokens], table[i])

    @pl.when(e == pl.num_programs(0) - 1)
    def _():
        for i in range(count):
            parts[2 * i][:cut, :] = acc[i * tokens:i * tokens + cut, :].astype(BF16)
            parts[2 * i][cut:, :] = jnp.zeros((experts_all, acc.shape[1]), BF16)
            parts[2 * i][cut:, :tokens] = table[i].astype(BF16)
            parts[2 * i + 1][...] = acc[i * tokens + cut:(i + 1) * tokens, :].astype(BF16)


def block_backward(first, xs, gs, routes, offsets, experts_all, w_gate, w_up, w_down):
    count = len(xs)
    tokens, width = xs[0].shape
    experts, _, each = w_gate.shape
    rows = count * tokens
    cut = tokens // 2

    def whole(shape):
        return pl.BlockSpec(shape, lambda e: (0,) * len(shape))

    def own(shape):
        return pl.BlockSpec((1,) + shape, lambda e: (e, 0, 0))

    def route_of(o):
        return pl.BlockSpec((1, 1, tokens), lambda e: (o * experts + e, 0, 0))

    halves = [(cut + experts_all, width), (tokens - cut, width)] * count
    outs = pl.pallas_call(
        functools.partial(block_kernel, count, tokens, cut),
        grid=(experts,),
        in_specs=[pl.BlockSpec(memory_space=pltpu.SMEM)]
        + [whole((tokens, width))] * (2 * count)
        + [route_of(o) for o in offsets]
        + [own((width, each)), own((width, each)), own((each, width))],
        out_specs=[whole(shape) for shape in halves]
        + [own((rows, each))] * 3,
        out_shape=[jax.ShapeDtypeStruct(shape, BF16) for shape in halves]
        + [jax.ShapeDtypeStruct((experts, rows, each), BF16)] * 3,
        scratch_shapes=[pltpu.VMEM((rows, width), F32), pltpu.VMEM((count, experts_all, tokens), F32)],
        compiler_params=pltpu.CompilerParams(dimension_semantics=("arbitrary",)),
        cost_estimate=pl.CostEstimate(
            flops=10 * rows * width * each * experts,
            bytes_accessed=6 * experts * width * each + 6 * rows * width,
            transcendentals=rows * each * experts,
        ),
        name="experts_block",
    )(first, *xs, *gs, *([routes] * count), w_gate, w_up, w_down)
    return outs[:2 * count], outs[2 * count:]


def update_kernel(talls, thins, parts, turned, *refs):
    tall_refs, thin_refs = refs[:talls], refs[talls:talls + thins * parts]
    outs, scratch = refs[talls + thins * parts:-1], refs[-1]

    @pl.when(pl.program_id(0) == 0)
    def _():
        tall = jnp.concatenate([ref[...] for ref in tall_refs], axis=0)
        scratch[...] = tall.T if turned else tall

    for p in range(parts):
        thin = jnp.concatenate([ref[0] for ref in thin_refs[p * thins:(p + 1) * thins]], axis=0)
        if turned:
            outs[p][0] = jnp.dot(scratch[...], thin, preferred_element_type=F32).astype(BF16)
        else:
            outs[p][0] = lax.dot_general(thin, scratch[...], ROWS, preferred_element_type=F32).astype(BF16)


def update(tall, thins, turned):
    count, parts = len(tall), len(thins)
    experts, _, each = thins[0][0].shape
    width = tall[0].shape[1]
    rows = sum(t.shape[0] for t in tall)
    shape = (width, each) if turned else (each, width)
    thin = [t for group in thins for t in group]
    return pl.pallas_call(
        functools.partial(update_kernel, count, len(thins[0]), parts, turned),
        grid=(experts,),
        in_specs=[pl.BlockSpec(t.shape, lambda e: (0, 0)) for t in tall]
        + [pl.BlockSpec((1,) + t.shape[1:], lambda e: (e, 0, 0)) for t in thin],
        out_specs=[pl.BlockSpec((1,) + shape, lambda e: (e, 0, 0))] * parts,
        out_shape=[jax.ShapeDtypeStruct((experts,) + shape, BF16)] * parts,
        scratch_shapes=[pltpu.VMEM((width, rows) if turned else (rows, width), BF16)],
        compiler_params=pltpu.CompilerParams(dimension_semantics=("arbitrary",)),
        cost_estimate=pl.CostEstimate(
            flops=2 * rows * width * each * experts * parts,
            bytes_accessed=2 * (rows * width + parts * experts * each * (rows + width)),
            transcendentals=0,
        ),
        name="weight_update",
    )(*tall, *thin)


def body(inputs, out_grads, expert_ids, route_levels, w_gate, w_up, w_down):
    x0, g0 = inputs[0], out_grads[0]
    ids = expert_ids[0]
    tokens, _ = x0.shape
    experts_local, _, _ = w_gate.shape[1:]
    groups = lax.axis_size("expert")
    experts_all = experts_local * groups
    half = groups // 2
    ring = ring_order(groups)
    fwd = [(ring[p], ring[(p + 1) % groups]) for p in range(groups)]
    bwd = [(b, a) for a, b in fwd]

    def go(value, pairs):
        return lax.ppermute(value, "expert", pairs)

    levels = route_levels[0].astype(F32) / 256.0
    catalog = jnp.arange(experts_all, dtype=jnp.int32)
    chosen = ids.T[None, :, :] == catalog[:, None, None]
    table = jnp.sum(jnp.where(chosen, levels.T[None], 0.0), axis=1).astype(BF16)
    received = lax.all_to_all(
        table.reshape(groups, experts_local, tokens), "expert", split_axis=0, concat_axis=0, tiled=True
    )
    ring_arr = jnp.array(ring, jnp.int32)
    me = lax.axis_index("expert")
    place = jnp.sum(jnp.where(ring_arr == me, jnp.arange(groups), 0))
    seat = jnp.sum(
        jnp.where(ring_arr[None, :] == jnp.arange(groups)[:, None], jnp.arange(groups)[None, :], 0), axis=1
    )
    turn = (
        jnp.mod(seat[None, :] - place, groups) == jnp.arange(groups)[:, None]
    ).astype(BF16)
    routes = jnp.dot(turn, received.reshape(groups, -1), preferred_element_type=F32)
    routes = routes.reshape(groups * experts_local, 1, tokens)
    first = (me * experts_local).astype(jnp.int32).reshape(1)

    xs, gs = {0: x0}, {0: g0}
    xf = xb = x0
    gf = gb = g0
    for hop in range(1, half + 1):
        xf = go(xf, fwd)
        gb = go(gb, bwd)
        xs[groups - hop], gs[hop] = xf, gb
        if hop < half:
            gf = go(gf, fwd)
            xb = go(xb, bwd)
            gs[groups - hop], xs[hop] = gf, xb

    low, high, tall_x, tall_g, thin = {}, {}, [], [], []
    for hop in range(half + 1):
        offsets = list(dict.fromkeys([hop, (groups - hop) % groups]))
        parts, grads = block_backward(
            first, [xs[o] for o in offsets], [gs[o] for o in offsets], routes, offsets, experts_all,
            w_gate[0], w_up[0], w_down[0],
        )
        for i, o in enumerate(offsets):
            low[o], high[o] = parts[2 * i], parts[2 * i + 1]
            tall_x.append(xs[o])
            tall_g.append(gs[o])
        thin.append(grads)

    def chain(pieces, pairs, offsets):
        carried = []
        for o in offsets:
            piece = pieces[o]
            if carried:
                piece = (carried[-1].astype(F32) + piece.astype(F32)).astype(BF16)
            carried.append(go(piece, pairs))
        return carried

    longer = list(range(half, 0, -1))
    forward_high = chain(high, fwd, longer[1:])
    backward_low = chain(low, bwd, [groups - o for o in longer[1:]])
    forward_low = chain(low, fwd, longer)
    backward_high = chain(high, bwd, [groups - o for o in longer])

    def total(own, one, two):
        return (own.astype(F32) + one[-1].astype(F32) + two[-1].astype(F32)).astype(BF16)

    low_total = total(low[0], forward_low, backward_low)
    cut = tokens // 2
    upstream = jnp.concatenate(
        [
            shifted(low_total[:cut], "section", -1),
            shifted(total(high[0], forward_high, backward_high), "section", -1),
        ],
        axis=0,
    )
    returned = low_total[cut:, :tokens].astype(F32)
    token_route = jnp.sum(jnp.where(chosen, returned[:, None, :], 0.0), axis=0).T.astype(BF16)

    gate_part, up_part = update(tall_x, [[t[0] for t in thin], [t[1] for t in thin]], True)
    (down_part,) = update(tall_g, [[t[2] for t in thin]], False)
    return (upstream[None], token_route[None], gate_part[None], up_part[None], down_part[None])


def solution(mesh):
    in_specs = (
        P("section", "expert", None),
        P("section", "expert", None),
        P("section", "expert", None),
        P("section", "expert", None),
        P("section", "expert", None, None),
        P("section", "expert", None, None),
        P("section", "expert", None, None),
    )
    out_specs = (
        P("section", "expert", None),
        P("section", "expert", None),
        P("section", "expert", None, None),
        P("section", "expert", None, None),
        P("section", "expert", None, None),
    )

    return jax.shard_map(body, mesh=mesh, in_specs=in_specs, out_specs=out_specs, check_vma=False)
```
